32 devices in a mesh: gx: 4 (over z), gy: 8 (over y, x, core).
Axes of the slice: x: 2, y: 2, z: 4, core: 2. Of those that a mesh axis runs over, the one named last changes fastest.
Arguments:
- substrates: float32 [8, 256, 128, 128], P(None, 'gx', 'gy'), may hold values from 0 to 2
- uptake: float32 [256, 128, 128], P('gx', 'gy'), may hold values from 0.5 to 2
- diffusion: float32 [8], replicated, may hold values from 0.1 to 0.15
- decay_rate: float32 [8], replicated, may hold values from 0.01 to 0.1
Outputs:
- advanced: float32 [8, 256, 128, 128], P(None, 'gx', 'gy')
The draws below stay inside these ranges and needn't reach their ends.
All inputs are finite; a program needn't handle non-finite values.
Results may differ from the reference program's by a relative error of at most 0.00002.
Values sent between devices are 32-bit elements; how exact they have to be, the bound alone decides.
A program may use at most 128 MiB of HBM per device.

```python
import math
import jax
import jax.numpy as jnp

S = 8
CX = 64
CY = 16
CZ = 128
SUBSTEPS = 4
NX = 256
NY = 128


def draw_substrates(key, part):
    first_key, second_key, third_key = jax.random.split(jax.random.fold_in(key, 17), 3)
    grid_shape = (S, NX, NY, CZ)
    x_local = jnp.arange(NX) % CX
    y_local = jnp.arange(NY) % CY
    x_band = (x_local < 4) | (x_local >= CX - 4)
    y_band = (y_local < 4) | (y_local >= CY - 4)
    in_band = (x_band[:, None] | y_band[None, :])[None, :, :, None]
    coin_flips = jax.random.randint(first_key, grid_shape, 0, 2).astype(jnp.float32)
    jitter_values = jax.random.uniform(second_key, grid_shape, jnp.float32)
    inside_draw = jax.random.uniform(third_key, grid_shape, jnp.float32)
    edge_values = 1.6 * coin_flips + 0.4 * jitter_values
    inside_values = 0.4 + 0.4 * inside_draw
    return jnp.where(in_band, edge_values, inside_values).astype(jnp.float32)


def block_scale(own_key, extent, cuts, least, largest):
    factor_of, own = 1.0, jax.random.fold_in(own_key, 6)
    for dim, blocks in cuts:
        steps = jnp.exp(jax.random.uniform(jax.random.fold_in(own, dim), (blocks,), jnp.float32, least / len(cuts), largest / len(cuts)))
        factor_of = factor_of * jnp.repeat(steps, extent[dim] // blocks).reshape([-1 if axis == dim else 1 for axis in range(len(extent))])
    return factor_of


def setup_inputs(seed: int = 0) -> dict:
    splits = jax.random.split(jax.random.key(seed), 5)
    return {
        "substrates": draw_substrates(jax.random.fold_in(splits[4], 71), 0),
        "uptake": jnp.clip(jnp.exp(math.log(2.0) - 1.3862944 * jax.random.uniform(splits[1], (NX, NY, CZ), jnp.float32) ** block_scale(splits[1], (NX, NY, CZ), ((0, 4), (1, 8)), -0.2, 0.2)), 0.5, 2.0),
        "diffusion": jnp.clip(jnp.exp(jax.random.uniform(splits[2], (S,), jnp.float32, math.log(0.1), math.log(0.15))), 0.1, 0.15),
        "decay_rate": jnp.clip(jnp.exp(jax.random.uniform(splits[3], (S,), jnp.float32, math.log(0.01), math.log(0.1))), 0.01, 0.1),
    }


def advance(concentration, uptake, diffuse, decays):
    laplace = jnp.roll(concentration, -1, 1) + jnp.roll(concentration, 1, 1)
    laplace = laplace + jnp.roll(concentration, -1, 2) + jnp.roll(concentration, 1, 2)
    laplace = laplace + jnp.roll(concentration, -1, 3) + jnp.roll(concentration, 1, 3)
    laplace = laplace - 6.0 * concentration
    return concentration + diffuse * laplace - decays * uptake[None] * concentration


def reference(substrates, uptake, diffusion, decay_rate):
    diffuse = diffusion[:, None, None, None]
    decays = decay_rate[:, None, None, None]
    concentration = substrates
    for substep in range(SUBSTEPS):
        concentration = advance(concentration, uptake, diffuse, decays)
    return concentration
```

```python
import functools

import jax
import jax.numpy as jnp
from jax import lax
from jax.experimental import pallas as pl
from jax.experimental.pallas import tpu as pltpu
from jax.sharding import PartitionSpec as P

SUBSTEPS = 4
PITCH_PAD = 16
Y0 = 8
MESH = pl.DeviceIdType.MESH


def kernel(
    n_x, n_y, sub_ref, up_ref, dif_ref, dec_ref, out_ref,
    field, uptake, result, faces, halos, load_sem, up_sem, store_sem, send_sem, recv_sem,
):
    count, cx, cy, cz = sub_ref.shape
    pitch = cy + PITCH_PAD
    rows = field.reshape(SUBSTEPS, count, (cx + 2) * pitch, cz)
    gx, gy = lax.axis_index("gx"), lax.axis_index("gy")
    low_x, high_x = lax.rem(gx + n_x - 1, n_x), lax.rem(gx + 1, n_x)
    low_y, high_y = lax.rem(gy + n_y - 1, n_y), lax.rem(gy + 1, n_y)
    inner = pl.ds(Y0, cy)

    def load(s):
        return pltpu.make_async_copy(
            sub_ref.at[s], field.at[0, s, pl.ds(1, cx), inner, :], load_sem.at[s]
        )

    def store(s):
        return pltpu.make_async_copy(result.at[s], out_ref.at[s], store_sem.at[s])

    def sends(t, s):
        here = field.at[t, s]
        pairs = (
            (faces.at[t, s, 0], halos.at[t, s, 0], (gx, low_y)),
            (faces.at[t, s, 1], halos.at[t, s, 1], (gx, high_y)),
            (here.at[1, inner, :], here.at[cx + 1, inner, :], (low_x, gy)),
            (here.at[cx, inner, :], here.at[0, inner, :], (high_x, gy)),
        )
        return [
            pltpu.make_async_remote_copy(
                src_ref=src, dst_ref=dst, send_sem=send_sem.at[t, s, k],
                recv_sem=recv_sem.at[t, s, k], device_id=target, device_id_type=MESH,
            )
            for k, (src, dst, target) in enumerate(pairs)
        ]

    def emit(t, s):
        for i in range(cx // 8):
            top = (1 + 8 * i) * pitch + Y0
            faces[t, s, 0, pl.ds(8 * i, 8), :] = rows[t, s, pl.ds(top, 8, stride=pitch), :]
            faces[t, s, 1, pl.ds(8 * i, 8), :] = rows[
                t, s, pl.ds(top + cy - 1, 8, stride=pitch), :
            ]
        for copy in sends(t, s):
            copy.start()

    def unit(t, s):
        for copy in sends(t, s):
            copy.wait_recv()
        for i in range(cx // 8):
            top = (1 + 8 * i) * pitch + Y0
            rows[t, s, pl.ds(top + cy, 8, stride=pitch), :] = halos[t, s, 0, pl.ds(8 * i, 8), :]
            rows[t, s, pl.ds(top - 1, 8, stride=pitch), :] = halos[t, s, 1, pl.ds(8 * i, 8), :]
        diffuse = dif_ref[s]
        keep = 1.0 - 6.0 * diffuse
        decay = dec_ref[s]
        block = 8

        def strip(b, carry):
            x0 = b * block
            for y in range(0, cy, 8):
                below = field[t, s, x0, pl.ds(Y0 + y, 8), :]
                center = field[t, s, x0 + 1, pl.ds(Y0 + y, 8), :]
                for i in range(block):
                    x = x0 + i
                    above = field[t, s, x + 2, pl.ds(Y0 + y, 8), :]
                    total = below + above
                    total = total + (
                        field[t, s, x + 1, pl.ds(Y0 + y - 1, 8), :]
                        + field[t, s, x + 1, pl.ds(Y0 + y + 1, 8), :]
                    )
                    total = total + (pltpu.roll(center, 1, 1) + pltpu.roll(center, cz - 1, 1))
                    factor = keep - decay * uptake[x, pl.ds(y, 8), :]
                    value = diffuse * total + factor * center
                    if t + 1 < SUBSTEPS:
                        field[t + 1, s, x + 1, pl.ds(Y0 + y, 8), :] = value
                    else:
                        result[s, x, pl.ds(y, 8), :] = value
                    below, center = center, above
            return carry

        lax.fori_loop(0, cx // block, strip, 0)

    each = functools.partial(lax.fori_loop, 0, count, init_val=0)

    def run(body):
        def wrapped(s, carry):
            body(s)
            return carry

        each(body_fun=wrapped)

    run(lambda s: load(s).start())
    up_copy = pltpu.make_async_copy(up_ref, uptake, up_sem)
    up_copy.start()
    barrier = pltpu.get_barrier_semaphore()
    for target in ((gx, low_y), (gx, high_y), (low_x, gy), (high_x, gy)):
        pl.semaphore_signal(barrier, inc=1, device_id=target, device_id_type=MESH)
    pl.semaphore_wait(barrier, 4)

    def first(s):
        load(s).wait()
        emit(0, s)

    run(first)
    up_copy.wait()
    for t in range(SUBSTEPS):

        def advance(s):
            unit(t, s)
            if t + 1 < SUBSTEPS:
                emit(t + 1, s)
            else:
                store(s).start()

        run(advance)

    def finish(s):
        for t in range(SUBSTEPS):
            for copy in sends(t, s):
                copy.wait_send()
        store(s).wait()

    run(finish)


def solution(mesh):
    n_x, n_y = mesh.shape["gx"], mesh.shape["gy"]

    def local(substrates, uptake, diffusion, decay_rate):
        count, cx, cy, cz = substrates.shape
        any_spec = pl.BlockSpec(memory_space=pl.ANY)
        smem_spec = pl.BlockSpec(memory_space=pltpu.SMEM)
        return pl.pallas_call(
            functools.partial(kernel, n_x, n_y),
            out_shape=jax.ShapeDtypeStruct(substrates.shape, substrates.dtype),
            in_specs=[any_spec, any_spec, smem_spec, smem_spec],
            out_specs=any_spec,
            scratch_shapes=[
                pltpu.VMEM((SUBSTEPS, count, cx + 2, cy + PITCH_PAD, cz), jnp.float32),
                pltpu.VMEM((cx, cy, cz), jnp.float32),
                pltpu.VMEM((count, cx, cy, cz), jnp.float32),
                pltpu.VMEM((SUBSTEPS, count, 2, cx, cz), jnp.float32),
                pltpu.VMEM((SUBSTEPS, count, 2, cx, cz), jnp.float32),
                pltpu.SemaphoreType.DMA((count,)),
                pltpu.SemaphoreType.DMA,
                pltpu.SemaphoreType.DMA((count,)),
                pltpu.SemaphoreType.DMA((SUBSTEPS, count, 4)),
                pltpu.SemaphoreType.DMA((SUBSTEPS, count, 4)),
            ],
            compiler_params=pltpu.CompilerParams(
                collective_id=0, has_side_effects=True, vmem_limit_bytes=62 * 1024 * 1024
            ),
        )(substrates, uptake, diffusion, decay_rate)

    placed = (P(None, "gx", "gy", None), P("gx", "gy", None), P(), P())
    return jax.shard_map(
        local, mesh=mesh, in_specs=placed, out_specs=P(None, "gx", "gy", None), check_vma=False
    )
```

```python
import functools

import jax
import jax.numpy as jnp
from jax import lax
from jax.experimental import pallas as pl
from jax.experimental.pallas import tpu as pltpu
from jax.sharding import PartitionSpec as P

SUBSTEPS = 4
PITCH_PAD = 16
Y0 = 8
MESH = pl.DeviceIdType.MESH


def kernel(
    n_x, n_y, sub_ref, up_ref, dif_ref, dec_ref, out_ref,
    field, uptake, result, faces, halos, load_sem, up_sem, store_sem, send_sem, recv_sem,
):
    count, cx, cy, cz = sub_ref.shape
    pitch = cy + PITCH_PAD
    rows = field.reshape(SUBSTEPS, count, (cx + 2) * pitch, cz)
    gx, gy = lax.axis_index("gx"), lax.axis_index("gy")
    low_x, high_x = lax.rem(gx + n_x - 1, n_x), lax.rem(gx + 1, n_x)
    low_y, high_y = lax.rem(gy + n_y - 1, n_y), lax.rem(gy + 1, n_y)
    inner = pl.ds(Y0, cy)

    def load(s):
        return pltpu.make_async_copy(
            sub_ref.at[s], field.at[0, s, pl.ds(1, cx), inner, :], load_sem.at[s]
        )

    def store(s):
        return pltpu.make_async_copy(result.at[s], out_ref.at[s], store_sem.at[s])

    def sends(t, s):
        here = field.at[t, s]
        pairs = (
            (faces.at[t, s, 0], halos.at[t, s, 0], (gx, low_y)),
            (faces.at[t, s, 1], halos.at[t, s, 1], (gx, high_y)),
            (here.at[1, inner, :], here.at[cx + 1, inner, :], (low_x, gy)),
            (here.at[cx, inner, :], here.at[0, inner, :], (high_x, gy)),
        )
        return [
            pltpu.make_async_remote_copy(
                src_ref=src, dst_ref=dst, send_sem=send_sem.at[t, s, k],
                recv_sem=recv_sem.at[t, s, k], device_id=target, device_id_type=MESH,
            )
            for k, (src, dst, target) in enumerate(pairs)
        ]

    def emit(t, s):
        for i in range(cx // 8):
            top = (1 + 8 * i) * pitch + Y0
            faces[t, s, 0, pl.ds(8 * i, 8), :] = rows[t, s, pl.ds(top, 8, stride=pitch), :]
            faces[t, s, 1, pl.ds(8 * i, 8), :] = rows[
                t, s, pl.ds(top + cy - 1, 8, stride=pitch), :
            ]
        for copy in sends(t, s):
            copy.start()

    def unit(t, s):
        for copy in sends(t, s):
            copy.wait_recv()
        for i in range(cx // 8):
            top = (1 + 8 * i) * pitch + Y0
            rows[t, s, pl.ds(top + cy, 8, stride=pitch), :] = halos[t, s, 0, pl.ds(8 * i, 8), :]
            rows[t, s, pl.ds(top - 1, 8, stride=pitch), :] = halos[t, s, 1, pl.ds(8 * i, 8), :]
        diffuse = dif_ref[s]
        keep = 1.0 - 6.0 * diffuse
        decay = dec_ref[s]
        block = cx

        def strip(b, carry):
            x0 = b * block
            for y in range(0, cy, 8):
                below = field[t, s, x0, pl.ds(Y0 + y, 8), :]
                center = field[t, s, x0 + 1, pl.ds(Y0 + y, 8), :]
                for i in range(block):
                    x = x0 + i
                    above = field[t, s, x + 2, pl.ds(Y0 + y, 8), :]
                    total = below + above
                    total = total + (
                        field[t, s, x + 1, pl.ds(Y0 + y - 1, 8), :]
                        + field[t, s, x + 1, pl.ds(Y0 + y + 1, 8), :]
                    )
                    total = total + (pltpu.roll(center, 1, 1) + pltpu.roll(center, cz - 1, 1))
                    factor = keep - decay * uptake[x, pl.ds(y, 8), :]
                    value = diffuse * total + factor * center
                    if t + 1 < SUBSTEPS:
                        field[t + 1, s, x + 1, pl.ds(Y0 + y, 8), :] = value
                    else:
                        result[s, x, pl.ds(y, 8), :] = value
                    below, center = center, above
            return carry

        lax.fori_loop(0, cx // block, strip, 0)

    each = functools.partial(lax.fori_loop, 0, count, init_val=0)

    def run(body):
        def wrapped(s, carry):
            body(s)
            return carry

        each(body_fun=wrapped)

    run(lambda s: load(s).start())
    up_copy = pltpu.make_async_copy(up_ref, uptake, up_sem)
    up_copy.start()
    barrier = pltpu.get_barrier_semaphore()
    for target in ((gx, low_y), (gx, high_y), (low_x, gy), (high_x, gy)):
        pl.semaphore_signal(barrier, inc=1, device_id=target, device_id_type=MESH)
    pl.semaphore_wait(barrier, 4)

    def first(s):
        load(s).wait()
        emit(0, s)

    run(first)
    up_copy.wait()
    for t in range(SUBSTEPS):

        def advance(s):
            unit(t, s)
            if t + 1 < SUBSTEPS:
                emit(t + 1, s)
            else:
                store(s).start()

        run(advance)

    def finish(s):
        for t in range(SUBSTEPS):
            for copy in sends(t, s):
                copy.wait_send()
        store(s).wait()

    run(finish)


def solution(mesh):
    n_x, n_y = mesh.shape["gx"], mesh.shape["gy"]

    def local(substrates, uptake, diffusion, decay_rate):
        count, cx, cy, cz = substrates.shape
        any_spec = pl.BlockSpec(memory_space=pl.ANY)
        hbm_spec = pl.BlockSpec(memory_space=pltpu.HBM)
        smem_spec = pl.BlockSpec(memory_space=pltpu.SMEM)
        return pl.pallas_call(
            functools.partial(kernel, n_x, n_y),
            out_shape=jax.ShapeDtypeStruct(substrates.shape, substrates.dtype),
            in_specs=[hbm_spec, hbm_spec, smem_spec, smem_spec],
            out_specs=any_spec,
            scratch_shapes=[
                pltpu.VMEM((SUBSTEPS, count, cx + 2, cy + PITCH_PAD, cz), jnp.float32),
                pltpu.VMEM((cx, cy, cz), jnp.float32),
                pltpu.VMEM((count, cx, cy, cz), jnp.float32),
                pltpu.VMEM((SUBSTEPS, count, 2, cx, cz), jnp.float32),
                pltpu.VMEM((SUBSTEPS, count, 2, cx, cz), jnp.float32),
                pltpu.SemaphoreType.DMA((count,)),
                pltpu.SemaphoreType.DMA,
                pltpu.SemaphoreType.DMA((count,)),
                pltpu.SemaphoreType.DMA((SUBSTEPS, count, 4)),
                pltpu.SemaphoreType.DMA((SUBSTEPS, count, 4)),
            ],
            compiler_params=pltpu.CompilerParams(
                collective_id=0, has_side_effects=True, vmem_limit_bytes=47 * 1024 * 1024
            ),
        )(substrates, uptake, diffusion, decay_rate)

    placed = (P(None, "gx", "gy", None), P("gx", "gy", None), P(), P())
    return jax.shard_map(
        local, mesh=mesh, in_specs=placed, out_specs=P(None, "gx", "gy", None), check_vma=False
    )
```

```python
import functools

import jax
import jax.numpy as jnp
from jax import lax
from jax.experimental import pallas as pl
from jax.experimental.pallas import tpu as pltpu
from jax.sharding import PartitionSpec as P

SUBSTEPS = 4
PITCH_PAD = 16
Y0 = 8
MESH = pl.DeviceIdType.MESH


def kernel(
    n_x, n_y, sub_ref, up_ref, dif_hbm, dec_hbm, out_ref,
    field, uptake, result, faces, halos, load_sem, up_sem, store_sem, send_sem, recv_sem,
    dif_ref, dec_ref, scalar_sem,
):
    count, cx, cy, cz = sub_ref.shape
    pitch = cy + PITCH_PAD
    rows = field.reshape(SUBSTEPS, count, (cx + 2) * pitch, cz)
    gx, gy = lax.axis_index("gx"), lax.axis_index("gy")
    low_x, high_x = lax.rem(gx + n_x - 1, n_x), lax.rem(gx + 1, n_x)
    low_y, high_y = lax.rem(gy + n_y - 1, n_y), lax.rem(gy + 1, n_y)
    inner = pl.ds(Y0, cy)

    def load(s):
        return pltpu.make_async_copy(
            sub_ref.at[s], field.at[0, s, pl.ds(1, cx), inner, :], load_sem.at[s]
        )

    def store(s):
        return pltpu.make_async_copy(result.at[s], out_ref.at[s], store_sem.at[s])

    def sends(t, s):
        here = field.at[t, s]
        pairs = (
            (faces.at[t, s, 0], halos.at[t, s, 0], (gx, low_y)),
            (faces.at[t, s, 1], halos.at[t, s, 1], (gx, high_y)),
            (here.at[1, inner, :], here.at[cx + 1, inner, :], (low_x, gy)),
            (here.at[cx, inner, :], here.at[0, inner, :], (high_x, gy)),
        )
        return [
            pltpu.make_async_remote_copy(
                src_ref=src, dst_ref=dst, send_sem=send_sem.at[t, s, k],
                recv_sem=recv_sem.at[t, s, k], device_id=target, device_id_type=MESH,
            )
            for k, (src, dst, target) in enumerate(pairs)
        ]

    def emit(t, s):
        for i in range(cx // 8):
            top = (1 + 8 * i) * pitch + Y0
            faces[t, s, 0, pl.ds(8 * i, 8), :] = rows[t, s, pl.ds(top, 8, stride=pitch), :]
            faces[t, s, 1, pl.ds(8 * i, 8), :] = rows[
                t, s, pl.ds(top + cy - 1, 8, stride=pitch), :
            ]
        for copy in sends(t, s):
            copy.start()

    def unit(t, s):
        for copy in sends(t, s):
            copy.wait_recv()
        for i in range(cx // 8):
            top = (1 + 8 * i) * pitch + Y0
            rows[t, s, pl.ds(top + cy, 8, stride=pitch), :] = halos[t, s, 0, pl.ds(8 * i, 8), :]
            rows[t, s, pl.ds(top - 1, 8, stride=pitch), :] = halos[t, s, 1, pl.ds(8 * i, 8), :]
        diffuse = dif_ref[s]
        keep = 1.0 - 6.0 * diffuse
        decay = dec_ref[s]
        block = cx

        def strip(b, carry):
            x0 = b * block
            for y in range(0, cy, 8):
                below = field[t, s, x0, pl.ds(Y0 + y, 8), :]
                center = field[t, s, x0 + 1, pl.ds(Y0 + y, 8), :]
                for i in range(block):
                    x = x0 + i
                    above = field[t, s, x + 2, pl.ds(Y0 + y, 8), :]
                    total = below + above
                    total = total + (
                        field[t, s, x + 1, pl.ds(Y0 + y - 1, 8), :]
                        + field[t, s, x + 1, pl.ds(Y0 + y + 1, 8), :]
                    )
                    total = total + (pltpu.roll(center, 1, 1) + pltpu.roll(center, cz - 1, 1))
                    factor = keep - decay * uptake[x, pl.ds(y, 8), :]
                    value = diffuse * total + factor * center
                    if t + 1 < SUBSTEPS:
                        field[t + 1, s, x + 1, pl.ds(Y0 + y, 8), :] = value
                    else:
                        result[s, x, pl.ds(y, 8), :] = value
                    below, center = center, above
            return carry

        lax.fori_loop(0, cx // block, strip, 0)

    each = functools.partial(lax.fori_loop, 0, count, init_val=0)

    def run(body):
        def wrapped(s, carry):
            body(s)
            return carry

        each(body_fun=wrapped)

    run(lambda s: load(s).start())
    up_copy = pltpu.make_async_copy(up_ref, uptake, up_sem)
    up_copy.start()
    scalar_copies = [
        pltpu.make_async_copy(dif_hbm, dif_ref, scalar_sem.at[0]),
        pltpu.make_async_copy(dec_hbm, dec_ref, scalar_sem.at[1]),
    ]
    for copy in scalar_copies:
        copy.start()
    barrier = pltpu.get_barrier_semaphore()
    for target in ((gx, low_y), (gx, high_y), (low_x, gy), (high_x, gy)):
        pl.semaphore_signal(barrier, inc=1, device_id=target, device_id_type=MESH)
    pl.semaphore_wait(barrier, 4)

    def first(s):
        load(s).wait()
        emit(0, s)

    run(first)
    up_copy.wait()
    for copy in scalar_copies:
        copy.wait()
    for t in range(SUBSTEPS):

        def advance(s):
            unit(t, s)
            if t + 1 < SUBSTEPS:
                emit(t + 1, s)
            else:
                store(s).start()

        run(advance)

    def finish(s):
        for t in range(SUBSTEPS):
            for copy in sends(t, s):
                copy.wait_send()
        store(s).wait()

    run(finish)


def solution(mesh):
    n_x, n_y = mesh.shape["gx"], mesh.shape["gy"]

    def local(substrates, uptake, diffusion, decay_rate):
        count, cx, cy, cz = substrates.shape
        any_spec = pl.BlockSpec(memory_space=pl.ANY)
        hbm_spec = pl.BlockSpec(memory_space=pltpu.HBM)
        return pl.pallas_call(
            functools.partial(kernel, n_x, n_y),
            out_shape=jax.ShapeDtypeStruct(substrates.shape, substrates.dtype),
            in_specs=[hbm_spec] * 4,
            out_specs=any_spec,
            scratch_shapes=[
                pltpu.VMEM((SUBSTEPS, count, cx + 2, cy + PITCH_PAD, cz), jnp.float32),
                pltpu.VMEM((cx, cy, cz), jnp.float32),
                pltpu.VMEM((count, cx, cy, cz), jnp.float32),
                pltpu.VMEM((SUBSTEPS, count, 2, cx, cz), jnp.float32),
                pltpu.VMEM((SUBSTEPS, count, 2, cx, cz), jnp.float32),
                pltpu.SemaphoreType.DMA((count,)),
                pltpu.SemaphoreType.DMA,
                pltpu.SemaphoreType.DMA((count,)),
                pltpu.SemaphoreType.DMA((SUBSTEPS, count, 4)),
                pltpu.SemaphoreType.DMA((SUBSTEPS, count, 4)),
                pltpu.SMEM((count,), jnp.float32),
                pltpu.SMEM((count,), jnp.float32),
                pltpu.SemaphoreType.DMA((2,)),
            ],
            compiler_params=pltpu.CompilerParams(
                collective_id=0, has_side_effects=True, vmem_limit_bytes=47 * 1024 * 1024
            ),
        )(*[pltpu.with_memory_space_constraint(v, pltpu.HBM) for v in (substrates, uptake, diffusion, decay_rate)])

    placed = (P(None, "gx", "gy", None), P("gx", "gy", None), P(), P())
    return jax.shard_map(
        local, mesh=mesh, in_specs=placed, out_specs=P(None, "gx", "gy", None), check_vma=False
    )
```
